32 devices in a mesh: row: 4 (over y, x), col: 8 (over z, core).
Axes of the slice: x: 2, y: 2, z: 4, core: 2. Of those that a mesh axis runs over, the one named last changes fastest.
Arguments:
- pair_states: bfloat16 [1024, 16384], P(None, ('row', 'col')), may hold values from -0.046875 to 0.046875
- screening: bfloat16 [4, 16384, 16384], P(None, 'row', 'col'), may hold values from -6 to 6
- qp_energy: float32 [8], replicated, may hold values from -0.5 to 0.5
- band_energy: float32 [2048], replicated, may hold values from -2 to 2
- band_index: int32 [128], replicated, may hold values from 0 to 2047
- nodes: float32 [4], replicated, may hold values from 0.1 to 2
- node_weights: float32 [4], replicated, may hold values from 0.05 to 1
Outputs:
- contrib: float32 [8, 128], replicated
- sigma: float32 [8], replicated
The draws below stay inside these ranges and needn't reach their ends.
All inputs are finite; a program needn't handle non-finite values.
Results may differ from the reference program's by a relative error of at most 0.0003.
Values may be sent and summed in bfloat16 or wider, within the bound.
A program may use at most 128 MiB of HBM per device.

```python
import math
import jax
import jax.numpy as jnp
from jax import lax

NG = 16384
FREQS = 4
NQ = 8
NM = 128
NBANDS = 2048
PAIRS = 1024


def plant(result, rng, least, top_value):
    dims = result.shape
    place = [jax.random.randint(jax.random.fold_in(rng, axis), (), 0, dims[axis]) for axis in range(len(dims))]
    result = result.at[tuple(place)].set(least)
    longest = dims.index(max(dims))
    place[longest] = (place[longest] + 1) % dims[longest]
    return result.at[tuple(place)].set(top_value)


def levels(rng, extent, cuts, least, largest):
    gain, own = 1.0, jax.random.fold_in(rng, 6)
    for axis_at, shards_of in cuts:
        heights = jnp.exp(jax.random.uniform(jax.random.fold_in(own, axis_at), (shards_of,), jnp.float32, least / len(cuts), largest / len(cuts)))
        gain = gain * jnp.repeat(heights, extent[axis_at] // shards_of).reshape([-1 if axis == axis_at else 1 for axis in range(len(extent))])
    return gain


def noise(rng, dims, width, reach, pieces=(), held_as=jnp.bfloat16):
    values = jax.random.normal(rng, dims, jnp.float32) * width
    if len(pieces) > 0:
        values = levels(rng, dims, pieces, -0.22, 0.18) * values
    return jnp.clip(values, min=-reach, max=reach).astype(held_as)


def setup_inputs(seed: int = 0) -> dict:
    key_of = jax.random.split(jax.random.key(seed), 8)
    return {
        "pair_states": noise(key_of[0], (PAIRS, NG), NG ** -0.5, 0.046875, ((1, 32),)),
        "screening": noise(key_of[1], (FREQS, NG, NG), 1.0, 6.0, ((1, 4), (2, 8))),
        "qp_energy": jnp.clip(jax.random.uniform(key_of[2], (NQ,), jnp.float32, -0.5, 0.5), -0.5, 0.5),
        "band_energy": jnp.clip(jax.random.uniform(key_of[3], (NBANDS,), jnp.float32, -2.0, 2.0), -2.0, 2.0),
        "band_index": plant(jax.random.randint(key_of[4], (NM,), 0, NBANDS), jax.random.fold_in(key_of[4], 1), 0, NBANDS - 1).astype(jnp.int32),
        "nodes": jnp.clip(jnp.exp(jax.random.uniform(key_of[5], (FREQS,), jnp.float32, math.log(0.1), math.log(2.0))), 0.1, 2.0),
        "node_weights": jnp.clip(jnp.exp(jax.random.uniform(key_of[6], (FREQS,), jnp.float32, math.log(0.05), math.log(1.0))), 0.05, 1.0),
    }


def reference(pair_states, screening, qp_energy, band_energy, band_index, nodes, node_weights):
    states = pair_states.astype(jnp.float32)

    def one_node(layer):
        image = jnp.dot(states, layer.astype(jnp.float32), precision=lax.Precision.HIGHEST, preferred_element_type=jnp.float32)
        return jnp.sum(image * states, axis=1)

    quad = lax.map(one_node, screening)
    table = jnp.arange(NBANDS).astype(jnp.int32)
    chosen = jnp.sum(jnp.where(band_index[:, None] == table[None, :], band_energy[None, :], jnp.float32(0.0)), axis=1)
    gap = (qp_energy[:, None] - chosen[None, :]).reshape(-1)
    factor = node_weights[:, None] * gap[None, :] / (gap[None, :] * gap[None, :] + nodes[:, None] * nodes[:, None])
    contrib = jnp.sum(factor * quad, axis=0).reshape(NQ, NM)
    sigma = jnp.sum(contrib, axis=1)
    return contrib, sigma
```

```python
import functools

import jax
import jax.numpy as jnp
from jax import lax
from jax.experimental import pallas as pl
from jax.experimental.pallas import tpu as pltpu
from jax.sharding import PartitionSpec as P

MESH = pl.DeviceIdType.MESH
CORES = 2
LANES = 128
RING = 4
CLOSE = 64

TAKE = {1: (4, 7, 9, 11), 2: (14, 16, 19, 20), 3: (24, 24, 28, 32)}
LATE = 99
PASS = (
    ((2, 4, 5, 6), (7, 10, 12, 14), (17, 19, 22, 23), (26, 27, 32, LATE)),
    ((4, 6, 7, 8), (10, 13, 15, 17), (20, 22, 25, 26), (28, 30, LATE, LATE)),
)


def kernel(
    rows, columns, own_ref, w_ref, qp_ref, band_ref, index_ref, nodes_ref, weights_ref, out_ref,
    panel, acc, tiles, qsum, fcol, chosen, near_sum, far_sum, qp, band, index, nodes, weights, taken, passed,
    small_sem, tile_sem, own_sem, r_send, r_recv, c_send, c_relay, c_recv, near_send, near_recv, far_send, far_recv,
):
    row, column = lax.axis_index("row"), lax.axis_index("col")
    chips = columns // CORES
    chip, core = column // CORES, column % CORES
    partner = column + 1 - 2 * core
    freqs, _, width = w_ref.shape
    pairs, depth = own_ref.shape
    parts = depth // LANES
    half = parts // 2
    steps = columns
    last = steps - 1
    units = steps * freqs + freqs
    bands = pairs // LANES
    held = columns * parts
    mine = width // LANES

    def at(r, c):
        return {"row": r, "col": c}

    home = chip
    side_x = home + 1 - 2 * (home % 2)
    side_y = (home + 2) % rows
    across = rows - 1 - home
    is_home = row == home
    ends = (chip == 0) | (chip == chips - 1)
    farthest = chips - 1 - chip
    is_x, is_y, is_far = row == side_x, row == side_y, row == across

    small = [
        pltpu.make_async_copy(src, dst, small_sem.at[i])
        for i, (src, dst) in enumerate(
            ((band_ref, band), (index_ref, index), (qp_ref, qp), (nodes_ref, nodes), (weights_ref, weights))
        )
    ]

    def rid(source, kind, part):
        return (source * CORES + kind) * parts + part

    def cid(source, kind, part):
        return ((source % CORES) * CORES + kind) * parts + part

    barrier = pltpu.get_barrier_semaphore()
    for other in range(1, columns):
        pl.semaphore_signal(barrier, inc=1, device_id=at(row, (column + other) % columns), device_id_type=MESH)
    for other in range(1, rows):
        for c in (column, partner):
            pl.semaphore_signal(barrier, inc=1, device_id=at((row + other) % rows, c), device_id_type=MESH)

    def own_copy(part):
        return pltpu.make_async_copy(
            own_ref.at[:, pl.ds(part * LANES, LANES)], panel.at[rid(chip, core, part)], own_sem.at[part]
        )

    for part in range(parts):
        own_copy(part).start()

    def source_of(step):
        j = step - 2
        edge = jnp.where(chip == 0, 1 + j // 2, chips - 2 - j // 2)
        inner = jnp.where(j < 4, chip - 1 + 2 * (j % 2), jnp.where(chip == 1, chips - 1, 0))
        source = jnp.where(ends, edge, inner)
        h = jnp.where(ends | (j >= 4), j % 2, j // 2)
        return source, h

    def blocks(step):
        source, h = source_of(step)
        first = step < 2
        kind = jnp.where(step == 1, 1 - core, core)
        a = jnp.where(first, rid(chip, kind, 0), rid(source, core, h * half))
        b = jnp.where(first, rid(chip, kind, half), rid(source, 1 - core, h * half))
        return a, b

    rows_of = half * LANES

    def tile_start(freq, pair):
        spot = freq % RING
        for place, block in enumerate(pair):
            pltpu.make_async_copy(
                w_ref.at[freq, pl.ds(pl.multiple_of(block * LANES, LANES), rows_of), :],
                tiles.at[spot, pl.ds(place * rows_of, rows_of), :],
                tile_sem.at[spot],
            ).start()

    def tile_wait(freq):
        spot = freq % RING
        pltpu.make_async_copy(tiles.at[spot], tiles.at[spot], tile_sem.at[spot]).wait()

    for freq in range(RING - 1):
        tile_start(freq, blocks(jnp.int32(0)))
    for copy in small:
        copy.start()

    def pass_on(source, part, way):
        slot = rid(source, core, part)
        target = [column + CORES, column - CORES, partner][way]
        return pltpu.make_async_remote_copy(
            src_ref=panel.at[slot], dst_ref=panel.at[slot], send_sem=r_send.at[way, source * parts + part],
            recv_sem=r_recv.at[slot], device_id=at(row, target), device_id_type=MESH,
        )

    def goes(source, way):
        if way == 0:
            return (source <= chip) & (chip < chips - 1)
        return (source >= chip) & (chip > 0)

    def c_first(source, part, side=0):
        slot = held + cid(source, core, part)
        return pltpu.make_async_remote_copy(
            src_ref=panel.at[rid(source, core, part)], dst_ref=panel.at[slot],
            send_sem=c_send.at[side, source * parts + part], recv_sem=c_recv.at[cid(source, core, part)],
            device_id=at(jnp.where(core == side, side_x, side_y), chip * CORES + source // CORES), device_id_type=MESH,
        )

    def c_next(kind, number):
        target = jnp.where(is_far, side_y if kind == 0 else side_x, across)
        return pltpu.make_async_remote_copy(
            src_ref=panel.at[held + number], dst_ref=panel.at[held + number], send_sem=c_relay.at[number],
            recv_sem=c_recv.at[number], device_id=at(target, column), device_id_type=MESH,
        )


    def relays(kind, source):
        return (is_far & (jnp.abs(source - chip) < chips - 1)) | (is_x if kind == 0 else is_y)

    def arrive(slot):
        pltpu.make_async_copy(panel.at[slot], panel.at[slot], r_recv.at[slot]).wait()

    def c_arrive(number):
        pltpu.make_async_copy(panel.at[held + number], panel.at[held + number], c_recv.at[number]).wait()

    def dispatch(source, part):
        for way in (0, 1):

            @pl.when(goes(source, way))
            def _():
                pass_on(source, part, way).start()

        pass_on(source, part, 2).start()

        @pl.when(is_home)
        def _():
            c_first(source, part).start()

    near_first = jnp.where(chip > core * CORES, 1, 0)
    wanted = [core * CORES + near_first, core * CORES + 1 - near_first]
    away = [jnp.abs(source - chip) for source in wanted]

    def due_at(order, part):
        value = jnp.int32(LATE)
        for distance in range(chips):
            there = jnp.where(is_far, PASS[1][distance][part], PASS[0][distance][part])
            value = jnp.where(away[order] == distance, there, value)
        return value

    due = [due_at(order, part) for order in range(2) for part in range(parts)]
    taken[units + 1] = jnp.int32(sum(map(len, TAKE.values())))
    for unit in range(units + 1):
        taken[unit] = jnp.int32(sum(take < unit for line in TAKE.values() for take in line))
        passed[unit] = sum((d < unit).astype(jnp.int32) for d in due)

    def wanted_at(order):
        return jnp.where(order == 0, wanted[0], wanted[1])

    def events(unit):
        @pl.loop(taken[unit], taken[unit + 1])
        def _(k):
            distance, part = 1 + k // parts, k % parts
            for source in (chip - distance, chip + distance):

                @pl.when((source >= 0) & (source < chips))
                def _():
                    arrive(rid(source, core, part))
                    dispatch(source, part)

        @pl.loop(passed[unit], passed[unit + 1])
        def _(k):
            for kind in range(CORES):

                @pl.when(relays(kind, wanted_at(k // parts)))
                def _():
                    number = cid(wanted_at(k // parts), kind, k % parts)
                    c_arrive(number)
                    c_next(kind, number).start()

        @pl.when(is_home & ends)
        def _():
            @pl.loop(taken[jnp.maximum(unit - 1, 0)], taken[unit])
            def _(k):
                @pl.when(k // parts == chips - 2)
                def _():
                    c_first(farthest, k % parts, 1).start()

    for copy in small:
        copy.wait()

    @pl.loop(0, LANES)
    def _(m):
        chosen[pl.ds(m, 1), :] = jnp.full((1, LANES), band[index[m]], jnp.float32)

    for freq in range(freqs):

        @pl.loop(0, bands)
        def _(n):
            gap = qp[n] - chosen[...]
            value = weights[freq] * gap / (gap * gap + nodes[freq] * nodes[freq])
            fcol[freq, pl.ds(pl.multiple_of(n * LANES, LANES), LANES), :] = value

    for part in range(parts):
        own_copy(part).wait()
    pl.semaphore_wait(barrier, columns - 1 + 2 * (rows - 1))
    for part in range(parts):
        dispatch(chip, part)

    def whole(freq, a, b):
        left = jnp.concatenate([panel[a + j] for j in range(half)] + [panel[b + j] for j in range(half)], axis=1)
        return jnp.dot(left, tiles[freq % RING], preferred_element_type=jnp.float32)

    def ahead(freq, pair, later):
        target = [jnp.where(freq == 0, now, then) for now, then in zip(pair, later)]
        tile_start((freq + RING - 1) % freqs, target)

    @pl.loop(0, freqs)
    def _(freq):
        events(freq)
        pair = blocks(jnp.int32(0))
        ahead(freq, pair, blocks(jnp.int32(1)))
        tile_wait(freq)
        acc[freq] = whole(freq, *pair)

    @pl.loop(1, last)
    def _(step):
        a, b = pair = blocks(step)
        later = blocks(step + 1)

        @pl.loop(0, freqs)
        def _(freq):
            events(step * freqs + freq)

            @pl.when(freq == 0)
            def _():
                @pl.when(step == 1)
                def _():
                    for j in range(half):
                        arrive(a + j)

                for j in range(half):
                    arrive(b + j)

            ahead(freq, pair, later)
            tile_wait(freq)
            acc[freq] += whole(freq, a, b)

    a, b = blocks(jnp.int32(last))
    for j in range(half):

        @pl.loop(0, freqs)
        def _(freq):
            events(last * freqs + j * freqs + freq)

            @pl.when(freq == 0)
            def _():
                arrive(b + j)

            if j == 0:

                @pl.when(freq == 0)
                def _():
                    tile_start(RING - 1, (a, b))

                tile_wait(freq)
            left = jnp.concatenate([panel[a + j], panel[b + j]], axis=1)
            spot = freq % RING
            right = jnp.concatenate(
                [tiles[spot, pl.ds(i * rows_of + j * LANES, LANES), :] for i in range(2)], axis=0
            )
            acc[freq] += jnp.dot(left, right, preferred_element_type=jnp.float32)

    base = jnp.where(is_home, core * mine, held)
    qsum[...] = jnp.zeros_like(qsum)

    def relay(order, part):
        for kind in range(CORES):

            @pl.when(relays(kind, wanted[order]) & (order * parts + part >= passed[units]))
            def _():
                number = cid(wanted[order], kind, part)
                c_arrive(number)
                c_next(kind, number).start()

    def collect(order, part):
        for kind in range(CORES):

            @pl.when(jnp.logical_not(is_home | relays(kind, wanted[order])))
            def _():
                c_arrive(cid(wanted[order], kind, part))

    def close(order, some):
        numbers = [cid(wanted[order], kind, part) for part in some for kind in range(CORES)]

        @pl.loop(0, pairs // CLOSE)
        def _(n):
            for i in range(0, CLOSE, 16):
                lines = pl.ds(pl.multiple_of(n * CLOSE, CLOSE) + i, 16)
                factors = [fcol[freq, lines, :] for freq in range(freqs)]
                value = qsum[lines, :]
                for number in numbers:
                    lanes = pl.ds(pl.multiple_of(number * LANES, LANES), LANES)
                    total = factors[0] * acc[0, lines, lanes]
                    for freq in range(1, freqs):
                        total = total + factors[freq] * acc[freq, lines, lanes]
                    value = value + total * panel[base + number, lines, :].astype(jnp.float32)
                qsum[lines, :] = value

    for order in range(2):
        for part in range(parts - order):
            relay(order, part)
    for part in range(parts):
        collect(0, part)
    close(0, range(parts))
    relay(1, parts - 1)
    for part in range(parts - 1):
        collect(1, part)
    close(1, range(parts - 1))
    collect(1, parts - 1)
    close(1, range(parts - 1, parts))

    sums = []
    for n in range(bands):
        sums.append(jnp.sum(qsum[pl.ds(n * LANES, LANES), :].T, axis=0, keepdims=True))
    near_sum[column] = jnp.concatenate(sums, axis=0)

    def near(other):
        return pltpu.make_async_remote_copy(
            src_ref=near_sum.at[column], dst_ref=near_sum.at[column], send_sem=near_send.at[other],
            recv_sem=near_recv.at[column], device_id=at(row, (column + other) % columns), device_id_type=MESH,
        )

    def far(other):
        return pltpu.make_async_remote_copy(
            src_ref=far_sum.at[row], dst_ref=far_sum.at[row], send_sem=far_send.at[other],
            recv_sem=far_recv.at[row], device_id=at((row + other) % rows, column), device_id_type=MESH,
        )

    for other in range(1, columns):
        near(other).start()
    for other in range(1, columns):
        slot = (column + other) % columns
        pltpu.make_async_copy(near_sum.at[slot], near_sum.at[slot], near_recv.at[slot]).wait()
    total = near_sum[0]
    for slot in range(1, columns):
        total = total + near_sum[slot]
    far_sum[row] = total
    for other in range(1, rows):
        far(other).start()
    for other in range(1, rows):
        slot = (row + other) % rows
        pltpu.make_async_copy(far_sum.at[slot], far_sum.at[slot], far_recv.at[slot]).wait()
    total = far_sum[0]
    for slot in range(1, rows):
        total = total + far_sum[slot]
    out_ref[...] = total

    for source in range(chips):

        @pl.loop(0, parts)
        def _(part):
            for way in (0, 1):

                @pl.when(goes(source, way))
                def _():
                    pass_on(source, part, way).wait_send()

            pass_on(source, part, 2).wait_send()

            @pl.when(is_home)
            def _():
                c_first(source, part).wait_send()

    @pl.when(is_home & ends)
    def _():
        @pl.loop(0, parts)
        def _(part):
            c_first(farthest, part, 1).wait_send()

    for kind in range(CORES):
        for order in range(2):

            @pl.when(relays(kind, wanted[order]))
            def _():
                @pl.loop(0, parts)
                def _(part):
                    c_next(kind, cid(wanted[order], kind, part)).wait_send()

    for other in range(1, rows):
        far(other).wait_send()
    for other in range(1, columns):
        near(other).wait_send()


def fused(pair_states, screening, qp_energy, band_energy, band_index, nodes, node_weights):
    rows, columns = lax.axis_size("row"), lax.axis_size("col")
    pairs, depth = pair_states.shape
    freqs, _, width = screening.shape
    shape = (qp_energy.shape[0], band_index.shape[0])
    parts = depth // LANES
    chips = columns // CORES
    mine = width // LANES
    dma = pltpu.SemaphoreType.DMA
    contrib = pl.pallas_call(
        functools.partial(kernel, rows, columns),
        out_shape=jax.ShapeDtypeStruct(shape, jnp.float32),
        in_specs=[pl.BlockSpec(memory_space=pl.ANY)] * 7,
        out_specs=pl.BlockSpec(memory_space=pltpu.VMEM),
        scratch_shapes=[
            pltpu.VMEM((columns * parts + mine, pairs, LANES), jnp.bfloat16),
            pltpu.VMEM((freqs, pairs, width), jnp.float32),
            pltpu.VMEM((RING, depth, width), jnp.bfloat16),
            pltpu.VMEM((pairs, LANES), jnp.float32),
            pltpu.VMEM((freqs, pairs, LANES), jnp.float32),
            pltpu.VMEM((LANES, LANES), jnp.float32),
            pltpu.VMEM((columns,) + shape, jnp.float32),
            pltpu.VMEM((rows,) + shape, jnp.float32),
            pltpu.SMEM(qp_energy.shape, jnp.float32),
            pltpu.SMEM(band_energy.shape, jnp.float32),
            pltpu.SMEM(band_index.shape, jnp.int32),
            pltpu.SMEM(nodes.shape, jnp.float32),
            pltpu.SMEM(node_weights.shape, jnp.float32),
            pltpu.SMEM((columns * freqs + freqs + 2,), jnp.int32),
            pltpu.SMEM((columns * freqs + freqs + 2,), jnp.int32),
            dma((5,)),
            dma((RING,)),
            dma((parts,)),
            dma((3, chips * parts)),
            dma((columns * parts,)),
            dma((2, chips * parts)),
            dma((mine,)),
            dma((mine,)),
            dma((columns,)),
            dma((columns,)),
            dma((rows,)),
            dma((rows,)),
        ],
        compiler_params=pltpu.CompilerParams(
            collective_id=0, has_side_effects=True, vmem_limit_bytes=67043328
        ),
        cost_estimate=pl.CostEstimate(
            flops=2 * freqs * pairs * columns * depth * width,
            bytes_accessed=freqs * columns * depth * width * 2,
            transcendentals=0,
        ),
    )(pair_states, screening, qp_energy, band_energy, band_index, nodes, node_weights)
    return contrib, jnp.sum(contrib, axis=1)


def broadcast(block, axis, holder):
    block = jnp.where(lax.axis_index(axis) == holder, block, jnp.zeros_like(block))
    return lax.psum(block, axis)


def shards(pair_states, screening, qp_energy, band_energy, band_index, nodes, node_weights):
    width = screening.shape[2]
    panel = lax.all_gather(pair_states, "col", axis=1, tiled=True)
    images = jnp.einsum("pg,fgc->fpc", panel, screening, preferred_element_type=jnp.float32)
    ratio = lax.axis_size("col") // lax.axis_size("row")
    column = lax.axis_index("col")
    offset = column % ratio * width
    own_piece = lax.dynamic_slice_in_dim(panel, offset, width, 1)
    col_states = broadcast(own_piece, "row", column // ratio)
    partial_value = jnp.sum(images * col_states.astype(jnp.float32)[None, :, :], axis=2)
    table = lax.broadcasted_iota(jnp.int32, (band_index.shape[0], band_energy.shape[0]), 1)
    chosen = jnp.sum(
        jnp.where(band_index[:, None] == table, band_energy[None, :], jnp.float32(0.0)), axis=1
    )
    gap = (qp_energy[:, None] - chosen[None, :]).reshape(-1)
    factor = (
        node_weights[:, None]
        * gap[None, :]
        / (gap[None, :] * gap[None, :] + nodes[:, None] * nodes[:, None])
    )
    flat = lax.psum(jnp.sum(factor * partial_value, axis=0), ("row", "col"))
    contrib = flat.reshape(qp_energy.shape[0], band_index.shape[0])
    sigma = jnp.sum(contrib, axis=1)
    return (contrib, sigma)


def step(pair_states, screening, *others):
    rows, columns = lax.axis_size("row"), lax.axis_size("col")
    pairs, depth = pair_states.shape
    freqs, _, width = screening.shape
    chips = columns // CORES
    held = pairs * ((columns * depth + width) * 2 + freqs * width * 4 + (freqs + 1) * LANES * 4)
    held = held + RING * depth * width * 2
    fits = depth == 4 * LANES and width == rows * depth and rows == 4 and chips == rows and columns % CORES == 0
    fits = fits and freqs == RING and others[2].shape[0] == LANES and pairs == others[0].shape[0] * LANES
    fits = fits and held < 60 * 2**20
    return (fused if fits else shards)(pair_states, screening, *others)


def solution(mesh):
    in_specs = (P(None, ("row", "col")), P(None, "row", "col"), P(), P(), P(), P(), P())
    out_specs = (P(), P())
    return jax.shard_map(step, mesh=mesh, in_specs=in_specs, out_specs=out_specs, check_vma=False)
```

```python
import functools

import jax
import jax.numpy as jnp
from jax import lax
from jax.experimental import pallas as pl
from jax.experimental.pallas import tpu as pltpu
from jax.sharding import PartitionSpec as P

MESH = pl.DeviceIdType.MESH
CORES = 2
LANES = 128
RING = 4
CLOSE = 256
PAIR = 2

TAKE = {1: (4, 6, 8, 10), 2: (14, 16, 18, 20), 3: (22, 26, 30, 34)}
LATE = 99
PASS = (
    ((2, 4, 4, 6), (8, 10, 12, 14), (18, 20, 22, 24), (26, 30, 34, 38)),
    ((4, 6, 8, 10), (10, 12, 14, 16), (22, 24, 26, 30), (30, 34, LATE, LATE)),
)


def kernel(
    rows, columns, own_ref, w_ref, qp_ref, band_ref, index_ref, nodes_ref, weights_ref, out_ref,
    panel, acc, tiles, qsum, fcol, chosen, total_of, qp, band, index, nodes, weights, taken, passed,
    small_sem, tile_sem, own_sem, r_send, r_recv, c_send, c_relay, c_recv, tell_send, tell_recv,
):
    row, column = lax.axis_index("row"), lax.axis_index("col")
    chips = columns // CORES
    chip, core = column // CORES, column % CORES
    partner = column + 1 - 2 * core
    freqs, _, width = w_ref.shape
    pairs, depth = own_ref.shape
    parts = depth // LANES
    half = parts // 2
    steps = columns
    last = steps - 1
    halved = last - 1
    units = (steps + steps - halved) * freqs
    bands = pairs // LANES
    held = columns * parts
    mine = width // LANES

    def at(r, c):
        return {"row": r, "col": c}

    home = chip
    side_x = home + 1 - 2 * (home % 2)
    side_y = (home + 2) % rows
    across = rows - 1 - home
    is_home = row == home
    ends = (chip == 0) | (chip == chips - 1)
    farthest = chips - 1 - chip
    is_x, is_y, is_far = row == side_x, row == side_y, row == across

    small = [
        pltpu.make_async_copy(src, dst, small_sem.at[i])
        for i, (src, dst) in enumerate(
            ((band_ref, band), (index_ref, index), (qp_ref, qp), (nodes_ref, nodes), (weights_ref, weights))
        )
    ]

    def rid(source, kind, part):
        return (source * CORES + kind) * parts + part

    def cid(source, kind, part):
        return ((source % CORES) * CORES + kind) * parts + part

    barrier = pltpu.get_barrier_semaphore()
    for other in range(1, columns):
        pl.semaphore_signal(barrier, inc=1, device_id=at(row, (column + other) % columns), device_id_type=MESH)
    for other in range(1, rows):
        for c in (column, partner):
            pl.semaphore_signal(barrier, inc=1, device_id=at((row + other) % rows, c), device_id_type=MESH)

    def own_copy(part):
        return pltpu.make_async_copy(
            own_ref.at[:, pl.ds(part * LANES, LANES)], panel.at[rid(chip, core, part)], own_sem.at[part]
        )

    for part in range(parts):
        own_copy(part).start()

    def source_of(step):
        j = step - 2
        edge = jnp.where(chip == 0, 1 + j // 2, chips - 2 - j // 2)
        inner = jnp.where(j < 4, chip - 1 + 2 * (j % 2), jnp.where(chip == 1, chips - 1, 0))
        source = jnp.where(ends, edge, inner)
        h = jnp.where(ends | (j >= 4), j % 2, j // 2)
        return source, h

    def blocks(step):
        source, h = source_of(step)
        first = step < 2
        kind = jnp.where(step == 1, 1 - core, core)
        a = jnp.where(first, rid(chip, kind, 0), rid(source, core, h * half))
        b = jnp.where(first, rid(chip, kind, half), rid(source, 1 - core, h * half))
        return a, b

    rows_of = half * LANES

    def tile_start(freq, pair):
        spot = freq % RING
        for place, block in enumerate(pair):
            pltpu.make_async_copy(
                w_ref.at[freq, pl.ds(pl.multiple_of(block * LANES, LANES), rows_of), :],
                tiles.at[spot, pl.ds(place * rows_of, rows_of), :],
                tile_sem.at[spot],
            ).start()

    def tile_wait(freq):
        spot = freq % RING
        pltpu.make_async_copy(tiles.at[spot], tiles.at[spot], tile_sem.at[spot]).wait()

    tile_start(0, blocks(jnp.int32(0)))

    def pass_on(source, part, way):
        slot = rid(source, core, part)
        target = [column + CORES, column - CORES, partner][way]
        return pltpu.make_async_remote_copy(
            src_ref=panel.at[slot], dst_ref=panel.at[slot], send_sem=r_send.at[way, source * parts + part],
            recv_sem=r_recv.at[slot], device_id=at(row, target), device_id_type=MESH,
        )

    def goes(source, way):
        if way == 0:
            return (source <= chip) & (chip < chips - 1)
        return (source >= chip) & (chip > 0)

    def c_first(source, part, side=0):
        slot = held + cid(source, core, part)
        return pltpu.make_async_remote_copy(
            src_ref=panel.at[rid(source, core, part)], dst_ref=panel.at[slot],
            send_sem=c_send.at[side, source * parts + part], recv_sem=c_recv.at[cid(source, core, part)],
            device_id=at(jnp.where(core == side, side_x, side_y), chip * CORES + source // CORES), device_id_type=MESH,
        )

    def c_next(kind, number):
        target = jnp.where(is_far, side_y if kind == 0 else side_x, across)
        return pltpu.make_async_remote_copy(
            src_ref=panel.at[held + number], dst_ref=panel.at[held + number], send_sem=c_relay.at[number],
            recv_sem=c_recv.at[number], device_id=at(target, column), device_id_type=MESH,
        )


    def relays(kind, source, part):
        return (is_far & ((jnp.abs(source - chip) < chips - 1) | (part < half))) | (is_x if kind == 0 else is_y)

    def arrive(slot):
        pltpu.make_async_copy(panel.at[slot], panel.at[slot], r_recv.at[slot]).wait()

    def c_arrive(number):
        pltpu.make_async_copy(panel.at[held + number], panel.at[held + number], c_recv.at[number]).wait()

    def dispatch(source, part):
        for way in (0, 1):

            @pl.when(goes(source, way))
            def _():
                pass_on(source, part, way).start()

        pass_on(source, part, 2).start()

        @pl.when(is_home)
        def _():
            c_first(source, part).start()

    near_first = jnp.where(chip > core * CORES, 1, 0)
    wanted = [core * CORES + near_first, core * CORES + 1 - near_first]
    away = [jnp.abs(source - chip) for source in wanted]

    def due_at(order, part):
        value = jnp.int32(LATE)
        for distance in range(chips):
            there = jnp.where(is_far, PASS[1][distance][part], PASS[0][distance][part])
            value = jnp.where(away[order] == distance, there, value)
        return value

    due = [due_at(order, part) for order in range(2) for part in range(parts)]
    taken[units + 1] = jnp.int32(sum(map(len, TAKE.values())))
    for unit in range(units + 1):
        taken[unit] = jnp.int32(sum(take < unit for line in TAKE.values() for take in line))
        passed[unit] = sum((d < unit).astype(jnp.int32) for d in due)

    def wanted_at(order):
        return jnp.where(order == 0, wanted[0], wanted[1])

    def events(unit):
        @pl.loop(taken[unit], taken[unit + 1])
        def _(k):
            distance, part = 1 + k // parts, k % parts
            for source in (chip - distance, chip + distance):

                @pl.when((source >= 0) & (source < chips))
                def _():
                    arrive(rid(source, core, part))
                    dispatch(source, part)

        @pl.loop(passed[unit], passed[unit + 1])
        def _(k):
            for kind in range(CORES):

                @pl.when(relays(kind, wanted_at(k // parts), k % parts))
                def _():
                    number = cid(wanted_at(k // parts), kind, k % parts)
                    c_arrive(number)
                    c_next(kind, number).start()

        @pl.when(is_home & ends)
        def _():
            @pl.loop(taken[jnp.maximum(unit - PAIR, 0)], taken[jnp.maximum(unit - 1, 0)])
            def _(k):
                @pl.when((k // parts == chips - 2) & (k % parts >= half))
                def _():
                    c_first(farthest, k % parts, 1).start()

    for part in range(parts):
        own_copy(part).wait()
    pl.semaphore_wait(barrier, columns - 1 + 2 * (rows - 1))
    for part in range(parts):
        dispatch(chip, part)
    tile_start(1, blocks(jnp.int32(0)))
    for copy in small:
        copy.start()

    def whole(freq, a, b):
        left = jnp.concatenate([panel[a + j] for j in range(half)] + [panel[b + j] for j in range(half)], axis=1)
        return jnp.dot(left, tiles[freq % RING], preferred_element_type=jnp.float32)

    def ahead(freq, pair, later):
        target = [jnp.where(freq == 0, now, then) for now, then in zip(pair, later)]
        for i in range(PAIR):
            tile_start((freq + i + PAIR) % freqs, target)

    @pl.loop(0, freqs, step=PAIR)
    def _(freq):
        for i in range(PAIR):
            events(freq + i)
        pair = blocks(jnp.int32(0))
        ahead(freq, pair, blocks(jnp.int32(1)))
        for i in range(PAIR):
            tile_wait(freq + i)
        for i in range(PAIR):
            acc[freq + i] = whole(freq + i, *pair)

    for copy in small:
        copy.wait()

    @pl.loop(0, LANES, step=16)
    def _(m):
        for i in range(16):
            chosen[pl.ds(m + i, 1), :] = jnp.full((1, LANES), band[index[m + i]], jnp.float32)

    @pl.loop(0, bands)
    def _(n):
        gap = qp[n] - chosen[...]
        square = gap * gap
        for freq in range(freqs):
            value = weights[freq] * gap / (square + nodes[freq] * nodes[freq])
            fcol[freq, pl.ds(pl.multiple_of(n * LANES, LANES), LANES), :] = value

    @pl.loop(1, halved)
    def _(step):
        a, b = pair = blocks(step)
        later = blocks(step + 1)

        @pl.loop(0, freqs, step=PAIR)
        def _(freq):
            for i in range(PAIR):
                events(step * freqs + freq + i)

            @pl.when(freq == 0)
            def _():
                @pl.when(step == 1)
                def _():
                    for j in range(half):
                        arrive(a + j)

                for j in range(half):
                    arrive(b + j)

            ahead(freq, pair, later)
            for i in range(PAIR):
                tile_wait(freq + i)
            for i in range(PAIR):
                acc[freq + i] += whole(freq + i, a, b)

    def left_of(pair, j):
        return jnp.concatenate([panel[block + j] for block in pair], axis=1)

    def right_of(freq, j, lanes):
        return jnp.concatenate(
            [tiles[freq % RING, pl.ds(i * rows_of + j * LANES, LANES), lanes] for i in range(2)], axis=0
        )

    pair, later = blocks(jnp.int32(halved)), blocks(jnp.int32(last))
    for turn, now in ((0, pair), (half, later)):
        for j in range(half if turn == 0 else half - 1):

            @pl.loop(0, freqs, step=PAIR)
            def _(freq):
                for i in range(PAIR):
                    events((halved + turn + j) * freqs + freq + i)

                @pl.when(freq == 0)
                def _():
                    arrive(now[1] + j)

                if j == 0:

                    @pl.when(freq == 0)
                    def _():
                        for i in range(PAIR):
                            tile_start(PAIR + i, now)

                    for i in range(PAIR):
                        tile_wait(freq + i)
                else:

                    @pl.when(freq > 0)
                    def _():
                        for i in range(PAIR):
                            tile_start(i, later)

                for i in range(PAIR):
                    acc[freq + i] += jnp.dot(
                        left_of(now, j), right_of(freq + i, j, slice(None)), preferred_element_type=jnp.float32
                    )

    base = jnp.where(is_home, core * mine, held)
    qsum[...] = jnp.zeros_like(qsum)

    def relay(order, part):
        for kind in range(CORES):

            @pl.when(relays(kind, wanted[order], part) & (order * parts + part >= passed[units]))
            def _():
                number = cid(wanted[order], kind, part)
                c_arrive(number)
                c_next(kind, number).start()

    def collect(order, part):
        for kind in range(CORES):

            @pl.when(jnp.logical_not(is_home | relays(kind, wanted[order], part)))
            def _():
                c_arrive(cid(wanted[order], kind, part))

    arrive(later[1] + half - 1)
    for order in range(2):
        ready = parts - order
        for part in range(ready):

            @pl.when(passed[units] <= order * parts + part)
            def _():
                relay(order, part)

            collect(order, part)

        @pl.loop(0, CORES)
        def _(kind):
            events((last + half) * freqs + order * CORES + kind)
            number = cid(wanted[order], kind, 0)
            lanes = pl.ds(pl.multiple_of(number * LANES, LANES), depth)
            for freq in range(freqs):
                value = acc[freq, :, lanes] + jnp.dot(
                    left_of(later, half - 1), right_of(freq, half - 1, lanes), preferred_element_type=jnp.float32
                )
                part_sum = value[:, :LANES] * panel[base + number].astype(jnp.float32)
                for part in range(1, ready):
                    piece = value[:, part * LANES : (part + 1) * LANES]
                    part_sum = part_sum + piece * panel[base + number + part].astype(jnp.float32)
                for part in range(ready, parts):
                    piece = fcol[freq] * value[:, part * LANES : (part + 1) * LANES]
                    spot = pl.ds(pl.multiple_of((number + part) * LANES, LANES), LANES)
                    if freq == 0:
                        acc[0, :, spot] = piece
                    else:
                        acc[0, :, spot] += piece
                qsum[...] += fcol[freq] * part_sum

    relay(1, parts - 1)
    collect(1, parts - 1)
    for kind in range(CORES):
        number = cid(wanted[1], kind, parts - 1)

        @pl.loop(0, pairs, step=CLOSE)
        def _(n):
            lines = pl.ds(pl.multiple_of(n, CLOSE), CLOSE)
            spot = pl.ds(pl.multiple_of(number * LANES, LANES), LANES)
            qsum[lines, :] += acc[0, lines, spot] * panel[base + number, lines, :].astype(jnp.float32)

    sums = []
    for n in range(bands):
        sums.append(jnp.sum(qsum[pl.ds(n * LANES, LANES), :].T, axis=0, keepdims=True))
    everyone = rows * columns
    linear = row * columns + column
    total_of[linear] = jnp.concatenate(sums, axis=0)

    def tell(other):
        target = (linear + other) % everyone
        return pltpu.make_async_remote_copy(
            src_ref=total_of.at[linear], dst_ref=total_of.at[linear], send_sem=tell_send,
            recv_sem=tell_recv, device_id=at(target // columns, target % columns), device_id_type=MESH,
        )

    @pl.loop(1, everyone)
    def _(other):
        tell(other).start()

    for source in range(chips):

        @pl.loop(0, parts)
        def _(part):
            for way in (0, 1):

                @pl.when(goes(source, way))
                def _():
                    pass_on(source, part, way).wait_send()

            pass_on(source, part, 2).wait_send()

            @pl.when(is_home)
            def _():
                c_first(source, part).wait_send()

    @pl.when(is_home & ends)
    def _():
        @pl.loop(half, parts)
        def _(part):
            c_first(farthest, part, 1).wait_send()

    for kind in range(CORES):
        for order in range(2):

            @pl.loop(0, parts)
            def _(part):
                @pl.when(relays(kind, wanted[order], part))
                def _():
                    c_next(kind, cid(wanted[order], kind, part)).wait_send()

    others = total_of.at[pl.ds(1, everyone - 1)]
    pltpu.make_async_copy(others, others, tell_recv).wait()
    for i in range(2):
        totals = [total_of[slot] for slot in range(i, everyone, 2)]
        while len(totals) > 1:
            totals = [one + two for one, two in zip(totals[::2], totals[1::2])]
        out_ref[i] = totals[0]
    pltpu.make_async_copy(others, others, tell_send).wait()


def fused(pair_states, screening, qp_energy, band_energy, band_index, nodes, node_weights):
    rows, columns = lax.axis_size("row"), lax.axis_size("col")
    pairs, depth = pair_states.shape
    freqs, _, width = screening.shape
    shape = (qp_energy.shape[0], band_index.shape[0])
    parts = depth // LANES
    chips = columns // CORES
    mine = width // LANES
    dma = pltpu.SemaphoreType.DMA
    halves = pl.pallas_call(
        functools.partial(kernel, rows, columns),
        out_shape=jax.ShapeDtypeStruct((2,) + shape, jnp.float32),
        in_specs=[pl.BlockSpec(memory_space=pl.ANY)] * 7,
        out_specs=pl.BlockSpec(memory_space=pltpu.VMEM),
        scratch_shapes=[
            pltpu.VMEM((columns * parts + mine, pairs, LANES), jnp.bfloat16),
            pltpu.VMEM((freqs, pairs, width), jnp.float32),
            pltpu.VMEM((RING, depth, width), jnp.bfloat16),
            pltpu.VMEM((pairs, LANES), jnp.float32),
            pltpu.VMEM((freqs, pairs, LANES), jnp.float32),
            pltpu.VMEM((LANES, LANES), jnp.float32),
            pltpu.VMEM((rows * columns,) + shape, jnp.float32),
            pltpu.SMEM(qp_energy.shape, jnp.float32),
            pltpu.SMEM(band_energy.shape, jnp.float32),
            pltpu.SMEM(band_index.shape, jnp.int32),
            pltpu.SMEM(nodes.shape, jnp.float32),
            pltpu.SMEM(node_weights.shape, jnp.float32),
            pltpu.SMEM(((columns + 2) * freqs + 2,), jnp.int32),
            pltpu.SMEM(((columns + 2) * freqs + 2,), jnp.int32),
            dma((5,)),
            dma((RING,)),
            dma((parts,)),
            dma((3, chips * parts)),
            dma((columns * parts,)),
            dma((2, chips * parts)),
            dma((mine,)),
            dma((mine,)),
            dma,
            dma,
        ],
        compiler_params=pltpu.CompilerParams(
            collective_id=0, has_side_effects=True, vmem_limit_bytes=67043328
        ),
        cost_estimate=pl.CostEstimate(
            flops=2 * freqs * pairs * columns * depth * width,
            bytes_accessed=freqs * columns * depth * width * 2,
            transcendentals=0,
        ),
    )(pair_states, screening, qp_energy, band_energy, band_index, nodes, node_weights)
    contrib = halves[0] + halves[1]
    return contrib, jnp.sum(contrib, axis=1)


def broadcast(block, axis, holder):
    block = jnp.where(lax.axis_index(axis) == holder, block, jnp.zeros_like(block))
    return lax.psum(block, axis)


def shards(pair_states, screening, qp_energy, band_energy, band_index, nodes, node_weights):
    width = screening.shape[2]
    panel = lax.all_gather(pair_states, "col", axis=1, tiled=True)
    images = jnp.einsum("pg,fgc->fpc", panel, screening, preferred_element_type=jnp.float32)
    ratio = lax.axis_size("col") // lax.axis_size("row")
    column = lax.axis_index("col")
    offset = column % ratio * width
    own_piece = lax.dynamic_slice_in_dim(panel, offset, width, 1)
    col_states = broadcast(own_piece, "row", column // ratio)
    partial_value = jnp.sum(images * col_states.astype(jnp.float32)[None, :, :], axis=2)
    table = lax.broadcasted_iota(jnp.int32, (band_index.shape[0], band_energy.shape[0]), 1)
    chosen = jnp.sum(
        jnp.where(band_index[:, None] == table, band_energy[None, :], jnp.float32(0.0)), axis=1
    )
    gap = (qp_energy[:, None] - chosen[None, :]).reshape(-1)
    factor = (
        node_weights[:, None]
        * gap[None, :]
        / (gap[None, :] * gap[None, :] + nodes[:, None] * nodes[:, None])
    )
    flat = lax.psum(jnp.sum(factor * partial_value, axis=0), ("row", "col"))
    contrib = flat.reshape(qp_energy.shape[0], band_index.shape[0])
    sigma = jnp.sum(contrib, axis=1)
    return (contrib, sigma)


def step(pair_states, screening, *others):
    rows, columns = lax.axis_size("row"), lax.axis_size("col")
    pairs, depth = pair_states.shape
    freqs, _, width = screening.shape
    chips = columns // CORES
    held = pairs * ((columns * depth + width) * 2 + freqs * width * 4 + (freqs + 1) * LANES * 4)
    held = held + RING * depth * width * 2
    fits = depth == 4 * LANES and width == rows * depth and rows == 4 and chips == rows and columns % CORES == 0
    fits = fits and freqs == RING and others[2].shape[0] == LANES and pairs == others[0].shape[0] * LANES
    fits = fits and held < 60 * 2**20
    return (fused if fits else shards)(pair_states, screening, *others)


def solution(mesh):
    in_specs = (P(None, ("row", "col")), P(None, "row", "col"), P(), P(), P(), P(), P())
    out_specs = (P(), P())
    return jax.shard_map(step, mesh=mesh, in_specs=in_specs, out_specs=out_specs, check_vma=False)
```
